32 devices in a mesh: gx: 8 (over z, y), gy: 4 (over x, core).
Axes of the slice: x: 2, y: 2, z: 4, core: 2. Of those that a mesh axis runs over, the one named last changes fastest.
Arguments:
- operators: float32 [8, 4, 1536, 1536], P('gx', 'gy'), may hold values from -0.15625 to 0.15625
- sources: float32 [8, 4, 5, 64, 128], P('gx', 'gy'), may hold values from -6 to 6
- source_rows: int32 [8, 4, 128], P('gx', 'gy'), may hold values from 0 to 1535
- batch_plan: int32 [5], replicated, may hold values from 0 to 4, each once
Outputs:
- traces: float32 [8, 4, 4, 64, 1536], P('gx', 'gy')
- basis: float32 [8, 4, 64, 1536], P('gx', 'gy')
- factor: float32 [64, 64], replicated
The draws below stay inside these ranges and needn't reach their ends.
Inputs may be any that keep to these rules, and one draw needn't show every extreme that they name: `batch_plan`: a permutation of the 5 source blocks.
All inputs are finite; a program needn't handle non-finite values.
Results may differ from the reference program's by a relative error of at most 0.0003.
Values sent between devices are 32-bit elements; how exact they have to be, the bound alone decides.
A program may use at most 64 MiB of HBM per device.

```python
import jax
import jax.numpy as jnp
from jax import lax

ORDER = 1536
COLS = 64
NB = 5
NSRC = 128
SUBX = 8
SUBY = 4
ROWS = 49152


def with_ends(drawn, own_key, smallest, top_value):
    dims = drawn.shape
    place = [jax.random.randint(jax.random.fold_in(own_key, axis), (), 0, dims[axis]) for axis in range(len(dims))]
    drawn = drawn.at[tuple(place)].set(smallest)
    longest = dims.index(max(dims))
    place[longest] = (place[longest] + 1) % dims[longest]
    return drawn.at[tuple(place)].set(top_value)


def shard_levels(stream_key, dims, split, least, top_value):
    loudness, own = 1.0, jax.random.fold_in(stream_key, 6)
    for axis_at, blocks in split:
        heights = jnp.exp(jax.random.uniform(jax.random.fold_in(own, axis_at), (blocks,), jnp.float32, least / len(split), top_value / len(split)))
        loudness = loudness * jnp.repeat(heights, dims[axis_at] // blocks).reshape([-1 if axis == axis_at else 1 for axis in range(len(dims))])
    return loudness


def gaussian(key, dims, width, most, split=(), kind=jnp.bfloat16):
    loudness = shard_levels(key, dims, split, -0.22, 0.18) if split else 1.0
    entries = jax.random.normal(key, dims, jnp.float32) * width * loudness
    return jnp.minimum(jnp.maximum(entries, -most), most).astype(kind)


def setup_inputs(seed: int = 0) -> dict:
    arg_keys = jax.random.split(jax.random.key(seed), 5)
    return {
        "operators": gaussian(arg_keys[0], (SUBX, SUBY, ORDER, ORDER), ORDER ** -0.5, 0.15625, ((0, 8), (1, 4)), jnp.float32),
        "sources": gaussian(arg_keys[1], (SUBX, SUBY, NB, COLS, NSRC), 1.0, 6.0, ((0, 8), (1, 4)), jnp.float32),
        "source_rows": with_ends(jax.random.randint(arg_keys[2], (SUBX, SUBY, NSRC), 0, ORDER), jax.random.fold_in(arg_keys[2], 1), 0, ORDER - 1).astype(jnp.int32),
        "batch_plan": jax.random.permutation(arg_keys[3], NB).astype(jnp.int32),
    }


def reference(operators, sources, source_rows, batch_plan):
    ordered = jnp.take(sources, batch_plan, axis=2)
    total_rows = NB * COLS
    half = ORDER // 2

    def column(west_all, col_index):

        def cell(south_in, row_index):
            trace_map = operators[col_index, row_index]
            source = ordered[col_index, row_index].reshape(total_rows, NSRC)
            placing = (source_rows[col_index, row_index][:, None] == jnp.arange(ORDER, dtype=jnp.int32)[None, :]).astype(jnp.float32)
            joined = jnp.concatenate([west_all[row_index], south_in], axis=1)
            outgoing = jnp.dot(joined.astype(jnp.float32), trace_map.astype(jnp.float32), precision=lax.Precision.HIGHEST, preferred_element_type=jnp.float32)
            outgoing = outgoing + jnp.dot(source.astype(jnp.float32), placing.astype(jnp.float32), precision=lax.Precision.HIGHEST, preferred_element_type=jnp.float32)
            return (outgoing[:, half:], outgoing)
        start = jnp.zeros((total_rows, half), jnp.float32)
        _, outs = lax.scan(cell, start, jnp.arange(SUBY, dtype=jnp.int32))
        return (outs[:, :, :half], outs)
    west_start = jnp.zeros((SUBY, total_rows, half), jnp.float32)
    _, grid = lax.scan(column, west_start, jnp.arange(SUBX, dtype=jnp.int32))
    grid = grid.reshape(SUBX, SUBY, NB, COLS, ORDER)
    first = grid[:, :, 0]
    traces = grid[:, :, 1:]
    gram = jnp.einsum('xyco,xydo->cd', first, first, precision=lax.Precision.HIGHEST) / ROWS
    lower = jnp.linalg.cholesky(gram)
    flat = jnp.transpose(first, (2, 0, 1, 3)).reshape(COLS, SUBX * SUBY * ORDER)
    solved = jax.scipy.linalg.solve_triangular(lower, flat, lower=True)
    basis = jnp.transpose(solved.reshape(COLS, SUBX, SUBY, ORDER), (1, 2, 0, 3))
    return (traces, basis, lower.T)
```

```python
import functools

import jax
import jax.numpy as jnp
from jax import lax
from jax.experimental import pallas as pl
from jax.experimental.pallas import tpu as pltpu
from jax.sharding import PartitionSpec as P

MESH = pl.DeviceIdType.MESH
PIECES = 2
EAST_CHUNKS = 3
SPLIT_ROWS = 64
BLOCK = 4


def two_terms(x):
    high = x.astype(jnp.bfloat16)
    return high, (x - high.astype(jnp.float32)).astype(jnp.bfloat16)


def three_terms(x):
    high = x.astype(jnp.bfloat16)
    rest = x - high.astype(jnp.float32)
    middle, low = two_terms(rest)
    return jnp.concatenate([high, middle, low], axis=0)


def full_dot(a, b, dims):
    return lax.dot_general(
        a, b, (dims, ((), ())), precision=lax.Precision.HIGHEST, preferred_element_type=jnp.float32
    )


def eliminated(both, columns):
    tiles = [both[i : i + 8] for i in range(0, columns, 8)]
    inside = lax.broadcasted_iota(jnp.int32, tiles[0].shape, 0)
    for start in range(0, columns, BLOCK):
        h = start // 8
        span = range(h, len(tiles))
        down = [
            {i: jnp.broadcast_to(tiles[i][:, start + u : start + u + 1], inside.shape) for i in span}
            for u in range(BLOCK)
        ]
        for u in range(BLOCK):
            s = (start + u) % 8
            line = tiles[h][s : s + 1]
            inverse = 1.0 / down[u][h][s : s + 1]
            heads = [down[v][h][s : s + 1] for v in range(BLOCK)]
            for i in span:
                f = down[u][i] * inverse
                if i == h:
                    f = jnp.where(inside > s, f, 0.0)
                tiles[i] = tiles[i] - f * line
                for v in range(u + 1, BLOCK):
                    down[v][i] = down[v][i] - f * heads[v]
    both = jnp.concatenate(tiles, axis=0)
    below = lax.broadcasted_iota(jnp.int32, both.shape, 0)
    lane = lax.broadcasted_iota(jnp.int32, both.shape, 1)
    pivots = jnp.sum(jnp.where(lane == below, both, 0.0), axis=1, keepdims=True)
    both = both / jnp.sqrt(pivots)
    return jnp.where((lane >= columns) | (lane >= below), both, 0.0)


def finish_kernel(pieces, out, spread, traces, basis, factor, basis_here, factor_here, sems):
    count, width, order = out.shape
    columns = spread.shape[0]
    kept = pltpu.make_async_copy(out.at[pl.ds(pieces, count - pieces)], traces, sems.at[0])
    kept.start()
    factor_here[...] = spread[:, :columns]
    last = pltpu.make_async_copy(factor_here, factor, sems.at[1])
    last.start()
    first = out[0:pieces].reshape(columns, order)
    basis_here[...] = full_dot(spread[:, columns:], first, ((1,), (0,)))
    solved = pltpu.make_async_copy(basis_here, basis, sems.at[2])
    solved.start()
    kept.wait()
    last.wait()
    solved.wait()


def kernel(
    scale, plan_hbm, sources_hbm, rows_hbm, w_hbm,
    out, spread,
    plan, sources, rows, w_all, w_high, w_low, placing, west, south, x_west, x_south,
    gathered, mine,
    in_sem, w_sem, west_sem, south_sem, east_sent, north_sent,
    gram_sent, gram_got, spread_sent, spread_got,
):
    col, row = lax.axis_index("gx"), lax.axis_index("gy")
    ncols, nrows = lax.axis_size("gx"), lax.axis_size("gy")
    total = ncols * nrows
    me = col * nrows + row
    count, width, order = out.shape
    half = order // 2
    columns = sources.shape[1]
    pieces = columns // width
    has_west, has_south = col > 0, row > 0
    has_east, has_north = col < ncols - 1, row < nrows - 1
    origin = me == 0
    root = 1
    is_root = me == root
    root_at = {"gx": root // nrows, "gy": root % nrows}
    east_at = {"gx": col + 1, "gy": row}
    north_at = {"gx": col, "gy": row + 1}

    piece = half // EAST_CHUNKS
    steps = order // SPLIT_ROWS

    def load(i):
        at = pl.ds(pl.multiple_of(i * SPLIT_ROWS, SPLIT_ROWS), SPLIT_ROWS)
        return pltpu.make_async_copy(w_hbm.at[at], w_all.at[at], w_sem.at[i])

    small = [
        pltpu.make_async_copy(a, b, in_sem.at[i])
        for i, (a, b) in enumerate([(rows_hbm, rows), (sources_hbm, sources), (plan_hbm, plan)])
    ]
    for copy in small:
        copy.start()

    first_step = jnp.where(has_west, 0, steps // 2)
    last_step = jnp.where(has_south, steps, steps // 2)

    @pl.loop(first_step, last_step)
    def _(i):
        load(i).start()

    barrier = pltpu.get_barrier_semaphore()

    def greet(here, at):
        @pl.when(here)
        def _():
            pl.semaphore_signal(barrier, inc=1, device_id=at, device_id_type=MESH)

    greet(has_east, east_at)
    greet(has_north, north_at)
    greet(has_west, {"gx": col - 1, "gy": row})
    greet(has_south, {"gx": col, "gy": row - 1})
    greet(jnp.logical_not(is_root), root_at)

    @pl.when(is_root)
    def _():
        @pl.loop(0, total)
        def _(d):
            @pl.when(d != me)
            def _():
                pl.semaphore_signal(
                    barrier, inc=1, device_id={"gx": d // nrows, "gy": d % nrows}, device_id_type=MESH
                )

    for copy in small:
        copy.wait()
    entries = rows.shape[1]
    spots = jnp.transpose(jnp.broadcast_to(rows[...].astype(jnp.float32), (entries, entries)))
    lanes = lax.broadcasted_iota(jnp.int32, (entries, entries), 1).astype(jnp.float32)
    for c in range(0, order, entries):
        placing[:, c : c + entries] = jnp.where(spots == lanes + float(c), 1.0, 0.0).astype(jnp.bfloat16)

    def east_copy(q, c, n):
        return pltpu.make_async_remote_copy(
            src_ref=out.at[q, :, pl.ds(c, n)], dst_ref=west.at[q, :, pl.ds(c, n)],
            send_sem=east_sent, recv_sem=west_sem.at[q * EAST_CHUNKS + c // n], device_id=east_at, device_id_type=MESH,
        )

    def north_copy(q, c, n):
        return pltpu.make_async_remote_copy(
            src_ref=out.at[q, :, pl.ds(half + c, n)], dst_ref=south.at[q, :, pl.ds(c, n)],
            send_sem=north_sent, recv_sem=south_sem.at[q], device_id=north_at, device_id_type=MESH,
        )

    def place(q):
        block = sources[plan[q // pieces], pl.ds(pl.multiple_of((q % pieces) * width, width), width), :]
        high, low = two_terms(block)
        both = jnp.dot(
            jnp.concatenate([high, low], axis=0), placing[...], preferred_element_type=jnp.float32
        )
        out[q] = both[:width] + both[width:]

    greeted = (
        has_east.astype(jnp.int32) + has_north.astype(jnp.int32)
        + has_west.astype(jnp.int32) + has_south.astype(jnp.int32)
    )
    place(0)

    @pl.when(jnp.logical_not(origin))
    def _():
        @pl.loop(1, count)
        def _(q):
            place(q)

        @pl.loop(first_step, last_step)
        def _(i):
            load(i).wait()
            at = pl.ds(pl.multiple_of(i * SPLIT_ROWS, SPLIT_ROWS), SPLIT_ROWS)
            w_high[at, :], w_low[at, :] = two_terms(w_all[at, :])

    pl.semaphore_wait(barrier, greeted + jnp.where(is_root, total - 1, 1))

    def send_whole(q):
        @pl.when(has_east)
        def _():
            for j in range(EAST_CHUNKS):
                east_copy(q, j * piece, piece).start()

        @pl.when(has_north)
        def _():
            north_copy(q, 0, half).start()

    @pl.when(origin)
    def _():
        send_whole(0)

        @pl.loop(1, count)
        def _(q):
            place(q)
            send_whole(q)

    def times(x, k, c, n):
        depth = x.shape[1]
        a = jnp.dot(x[...], w_high[k : k + depth, c : c + n], preferred_element_type=jnp.float32)
        b = jnp.dot(x[:width, :], w_low[k : k + depth, c : c + n], preferred_element_type=jnp.float32)
        return a[:width] + (a[width:] + b)

    def gram_copy():
        return pltpu.make_async_remote_copy(
            src_ref=mine, dst_ref=gathered.at[me], send_sem=gram_sent, recv_sem=gram_got,
            device_id=root_at, device_id_type=MESH,
        )

    def partial_gram():
        first = out[0:pieces].reshape(columns, order)
        terms = three_terms(first)
        g = lax.dot_general(
            terms, terms, (((1,), (1,)), ((), ())), preferred_element_type=jnp.float32
        )
        g = (g[2 * columns :] + g[columns : 2 * columns]) + g[:columns]
        g = (g[:, 2 * columns :] + g[:, columns : 2 * columns]) + g[:, :columns]
        g = jnp.concatenate([g[: columns // 2], g[columns // 2 :]], axis=1)

        @pl.when(is_root)
        def _():
            gathered[me] = g

        @pl.when(jnp.logical_not(is_root))
        def _():
            mine[...] = g
            gram_copy().start()

    @pl.when(jnp.logical_not(origin))
    def _():
        @pl.loop(0, count)
        def _(q):
            @pl.when(has_south)
            def _():
                north_copy(q, 0, half).wait_recv()
                x_south[:width], x_south[width:] = two_terms(south[q])
                out[q] += times(x_south, half, 0, order)

            @pl.when(has_west)
            def _():
                for j in range(EAST_CHUNKS):
                    at = slice(j * piece, (j + 1) * piece)
                    east_copy(q, j * piece, piece).wait_recv()
                    x_west[:width, at], x_west[width:, at] = two_terms(west[q, :, at])
                    out[q, :, :half] += times(x_west.at[:, at], j * piece, 0, half)

                @pl.when(has_east)
                def _():
                    for j in range(EAST_CHUNKS):
                        east_copy(q, j * piece, piece).start()

                out[q, :, half:] += times(x_west, 0, half, half)

                @pl.when(has_north)
                def _():
                    north_copy(q, 0, half).start()

            @pl.when(jnp.logical_not(has_west))
            def _():
                send_whole(q)

            @pl.when(q == pieces - 1)
            def _():
                partial_gram()

    @pl.when(origin)
    def _():
        partial_gram()

    def spread_copy(d):
        return pltpu.make_async_remote_copy(
            src_ref=spread, dst_ref=spread, send_sem=spread_sent, recv_sem=spread_got,
            device_id={"gx": d // nrows, "gy": d % nrows}, device_id_type=MESH,
        )

    @pl.when(is_root)
    def _():
        pltpu.make_async_remote_copy(
            src_ref=gathered.at[pl.ds(0, total - 1)], dst_ref=gathered.at[pl.ds(0, total - 1)],
            send_sem=gram_sent, recv_sem=gram_got, device_id=east_at, device_id_type=MESH,
        ).wait_recv()
        summed = lax.fori_loop(
            1, total, lambda d, s: s + gathered[d], gathered[0]
        ) * scale
        gram = jnp.concatenate([summed[:, :columns], summed[:, columns:]], axis=0)
        i = lax.broadcasted_iota(jnp.int32, (columns, columns), 0)
        j = lax.broadcasted_iota(jnp.int32, (columns, columns), 1)
        both = jnp.concatenate([gram, jnp.where(i == j, 1.0, 0.0)], axis=1)
        spread[...] = eliminated(both, columns)

        @pl.loop(1, total)
        def _(t):
            spread_copy((root + total - t) % total).start()

    @pl.when(jnp.logical_not(is_root))
    def _():
        spread_copy(root).wait_recv()

    @pl.when(is_root)
    def _():
        pltpu.make_async_remote_copy(
            src_ref=gathered.at[pl.ds(0, 2 * (total - 1))], dst_ref=gathered.at[pl.ds(0, 2 * (total - 1))],
            send_sem=spread_sent, recv_sem=spread_got, device_id=east_at, device_id_type=MESH,
        ).wait_send()

    @pl.when(jnp.logical_not(is_root))
    def _():
        gram_copy().wait_send()

    @pl.when(has_east)
    def _():
        pltpu.make_async_remote_copy(
            src_ref=out.at[:, :, pl.ds(0, half)], dst_ref=west,
            send_sem=east_sent, recv_sem=west_sem.at[0], device_id=east_at, device_id_type=MESH,
        ).wait_send()

    @pl.when(has_north)
    def _():
        pltpu.make_async_remote_copy(
            src_ref=out.at[:, :, pl.ds(half, half)], dst_ref=south,
            send_sem=north_sent, recv_sem=south_sem.at[0], device_id=north_at, device_id_type=MESH,
        ).wait_send()


def body(operators, sources, source_rows, batch_plan):
    _, _, batches, columns, entries = sources.shape
    order = operators.shape[-1]
    half = order // 2
    width = columns // PIECES
    count = batches * PIECES
    total = lax.axis_size("gx") * lax.axis_size("gy")
    f32, bf16, dma = jnp.float32, jnp.bfloat16, pltpu.SemaphoreType.DMA
    vmem = pl.BlockSpec(memory_space=pltpu.VMEM)
    hbm = pl.BlockSpec(memory_space=pltpu.HBM)
    out, spread = pl.pallas_call(
        functools.partial(kernel, 1.0 / (total * order)),
        out_shape=(
            jax.ShapeDtypeStruct((count, width, order), f32),
            jax.ShapeDtypeStruct((columns, 2 * columns), f32),
        ),
        in_specs=[hbm, hbm, hbm, hbm],
        out_specs=(vmem, vmem),
        scratch_shapes=[
            pltpu.SMEM((batches,), jnp.int32),
            pltpu.VMEM((batches, columns, entries), f32),
            pltpu.VMEM((1, entries), jnp.int32),
            pltpu.VMEM((order, order), f32),
            pltpu.VMEM((order, order), bf16),
            pltpu.VMEM((order, order), bf16),
            pltpu.VMEM((entries, order), bf16),
            pltpu.VMEM((count, width, half), f32),
            pltpu.VMEM((count, width, half), f32),
            pltpu.VMEM((2 * width, half), bf16),
            pltpu.VMEM((2 * width, half), bf16),
            pltpu.VMEM((2 * total, columns // 2, 2 * columns), f32),
            pltpu.VMEM((columns // 2, 2 * columns), f32),
            dma((3,)), dma((order // SPLIT_ROWS,)),
            dma((count * EAST_CHUNKS,)), dma((count,)), dma, dma, dma, dma, dma, dma,
        ],
        compiler_params=pltpu.CompilerParams(
            collective_id=0, has_side_effects=True, vmem_limit_bytes=48 * 1024 * 1024
        ),
        name="sweep",
    )(*[pltpu.with_memory_space_constraint(a, pltpu.HBM) for a in (batch_plan, sources[0, 0], source_rows[0], operators[0, 0])])
    traces, basis, factor = pl.pallas_call(
        functools.partial(finish_kernel, PIECES),
        out_shape=(
            jax.ShapeDtypeStruct((count - PIECES, width, order), f32),
            jax.ShapeDtypeStruct((columns, order), f32),
            jax.ShapeDtypeStruct((columns, columns), f32),
        ),
        in_specs=[vmem, vmem],
        out_specs=(hbm, hbm, hbm),
        scratch_shapes=[pltpu.VMEM((columns, order), f32), pltpu.VMEM((columns, columns), f32), dma((3,))],
        compiler_params=pltpu.CompilerParams(vmem_limit_bytes=8 * 1024 * 1024),
        name="finish",
    )(out, spread)
    return traces.reshape(1, 1, batches - 1, columns, order), basis[None, None], factor


def solution(mesh):
    return jax.shard_map(
        body,
        mesh=mesh,
        in_specs=(
            P("gx", "gy", None, None),
            P("gx", "gy", None, None, None),
            P("gx", "gy", None),
            P(),
        ),
        out_specs=(P("gx", "gy", None, None, None), P("gx", "gy", None, None), P()),
        check_vma=False,
    )
```
